32 devices in a mesh: section: 4 (over z), expert: 4 (over y, x), dp: 2 (over core).
Axes of the slice: x: 2, y: 2, z: 4, core: 2. Of those that a mesh axis runs over, the one named last changes fastest.
Arguments:
- stash: bfloat16 [4, 256, 2048], P('section', 'dp', 'expert'), may hold values from -6 to 6
- cotangent: bfloat16 [4, 256, 2048], P('section', 'dp', 'expert'), may hold values from -6 to 6
- backward_expert_routes: int32 [4, 256, 2], P('section', 'dp'), may hold values from 0 to 3, all different within a row; in each aligned block of 128 rows (0 to 127, 128 to 255, ..., all dimensions but the last counted through in order) at most 80 rows name the same one
- backward_job_lengths: int32 [4, 4], P('section'), may hold values from 1 to 128, 256 in all within a row
- layer_norm_gains: float32 [4, 2048], P('section'), may hold values from 0.25 to 1.75
- router: bfloat16 [4, 2048, 4], P('section'), may hold values from -0.125 to 0.125
- expert_gate_weight: bfloat16 [4, 2048, 28672], P('section', None, ('expert', 'dp')), may hold values from -0.125 to 0.125
- expert_up_weight: bfloat16 [4, 2048, 28672], P('section', None, ('expert', 'dp')), may hold values from -0.125 to 0.125
- expert_down_weight: bfloat16 [4, 28672, 2048], P('section', ('expert', 'dp')), may hold values from -0.0625 to 0.0625
- adapter_down_maps: bfloat16 [4, 2048, 64], P('section', 'expert'), may hold values from -0.125 to 0.125
- adapter_up_maps: bfloat16 [4, 64, 2048], P('section', None, 'expert'), may hold values from -1.5 to 1.5
Outputs:
- handed_back: bfloat16 [4, 256, 2048], P('section', 'dp', 'expert')
- grad_lora_down: float32 [4, 2048, 64], P('section', 'expert')
- grad_lora_up: float32 [4, 64, 2048], P('section', None, 'expert')
The draws below stay inside these ranges and needn't reach their ends.
Inputs may be any that keep to these rules, and one draw needn't show every extreme that they name: `backward_expert_routes`: each row names two different experts. In each aligned block of 128 rows (the tokens of one device) no expert is named more than 80 times. `backward_job_lengths`: each row sums to 256.
All inputs are finite; a program needn't handle non-finite values.
Results may differ from the reference program's by a relative error of at most 0.008.
Values may be sent and summed in bfloat16 or wider, within the bound.
A program may use at most 128 MiB of HBM per device.

```python
import math
import jax
import jax.numpy as jnp
import numpy as np
from jax import lax

MODEL_WIDTH = 2048
FF = 7168
EXPERTS = 4
TOP = 2
ADAPTER_RANK = 16
ADAPTER_JOBS = 4
TOK_DEV = 128
CAP = 80
TOKENS = 256
LAYER_COUNT = 4


def levels(rng, dims, split, low, top_value):
    def one(dim, blocks):
        steps = jax.random.uniform(jax.random.fold_in(jax.random.fold_in(rng, 6), dim), (blocks,), jnp.float32, low / len(split), top_value / len(split))
        return jnp.repeat(jnp.exp(steps), dims[dim] // blocks).reshape((-1,) + (1,) * (len(dims) - dim - 1))

    level = one(*split[0])
    for cut in split[1:]:
        level = level * one(*cut)
    return level


def profile(count, total, reach, lean):
    weights = [(1 << 20) // math.isqrt(rank ** lean) + 1 for rank in range(2, count + 1)]
    spare, given = total - reach - (count - 1), [1] * (count - 1)
    while spare > 0:
        candidates = [i for i in range(count - 1) if given[i] < reach]
        pool, budget = sum([weights[i] for i in candidates]), spare
        for i in candidates:
            extra = min(reach - given[i], max(1, budget * weights[i] // pool), spare)
            given[i] = given[i] + extra
            spare = spare - extra
    return np.array([reach] + given)


def uneven(rng, number_of, total, reach, lean):
    if number_of == 2:
        one = jax.random.randint(rng, (), max(1, total - reach), min(reach, total - 1) + 1)
        return jnp.stack([one, total - one])
    lengths = jnp.asarray(profile(number_of, total, reach, lean), jnp.int32)
    twos = (number_of - 1) // 2
    giver, taker = lengths[1:1 + 2 * twos:2], lengths[2:2 + 2 * twos:2]
    margin = jnp.minimum(giver - 1, reach - taker)
    passed = jax.random.randint(jax.random.fold_in(rng, 1), (twos,), 0, 1 << 20) % (margin + 1)
    lengths = lengths.at[1:1 + 2 * twos:2].set(giver - passed).at[2:2 + 2 * twos:2].set(taker + passed)
    return lengths[jax.random.permutation(jax.random.fold_in(rng, 2), number_of)]


def shared_out(key, own, number, rows, amount, top, limit, slope):
    ranking = jax.random.permutation(key, amount)
    heavy_load, ordinary = shares(amount, rows * top, limit, slope, True), shares(amount, rows * top, limit, slope, False)
    places = jnp.arange(amount)

    def named(sizes, rotation):
        used = int((sizes > 0).sum())
        fixed = max(1, used // 4)
        passed = fixed + (places - fixed + rotation * (used - fixed)) % max(1, amount - fixed)
        return jnp.zeros((amount,), jnp.int32).at[ranking[jnp.where(places < fixed, places, passed)]].set(jnp.asarray(sizes, jnp.int32))

    sizes = jnp.where(number % 4 == 0, named(heavy_load, number // 4), named(ordinary, number - number // 4 - 1))
    mixed = jax.random.permutation(jax.random.fold_in(own, 3), amount)
    donor, taker = mixed[0:amount // 2 * 2:2], mixed[1:amount // 2 * 2:2]
    room = jnp.minimum(sizes[donor] - 1, limit - sizes[taker]) // 2
    room = jnp.where((donor == ranking[0]) | (taker == ranking[0]) | (sizes[taker] == 0), 0, jnp.maximum(room, 0))
    passed = jax.random.randint(jax.random.fold_in(own, 4), (amount // 2,), 0, 1 << 20) % (room + 1)
    sizes = sizes.at[donor].add(-passed).at[taker].add(passed)
    items = jnp.searchsorted(jnp.cumsum(sizes), jnp.arange(rows * top), side="right").astype(jnp.int32)
    grid = items.reshape(top, rows).T
    grid = grid[jax.random.permutation(jax.random.fold_in(own, 1), rows)]
    rotation = jax.random.randint(jax.random.fold_in(own, 2), (rows, 1), 0, top)
    return jnp.take_along_axis(grid, (jnp.arange(top)[None, :] + rotation) % top, axis=1)


def shares(number_of, total, limit, slope, full):
    loads = [(1 << 20) // math.isqrt(standing ** slope) + 1 for standing in range(1, number_of + 1)]
    largest = limit if full else min(limit, max(-(-total // number_of), total * loads[0] // sum(loads)))
    least = 1 if total - largest >= number_of - 1 else 0
    holding, spare = [largest] + [least] * (number_of - 1), total - largest - least * (number_of - 1)
    while spare > 0:
        candidates = [i for i in range(1, number_of) if holding[i] < largest] or [i for i in range(1, number_of) if holding[i] < limit]
        whole, left = sum([loads[i] for i in candidates]), spare
        for i in candidates:
            addition = min(limit - holding[i], max(1, left * loads[i] // whole), spare)
            holding[i] = holding[i] + addition
            spare = spare - addition
    return np.array(holding)


def centred(own_key, extent, scale, bound, pieces=(), held_as=jnp.bfloat16):
    array = scale * jax.random.normal(own_key, extent, jnp.float32)
    if pieces:
        array = array * levels(own_key, extent, pieces, -0.22, 0.18)
    return jnp.clip(array, -bound, bound).astype(held_as)


def setup_inputs(seed: int = 0) -> dict:
    key_of = jax.random.split(jax.random.key(seed), 12)
    stash = centred(key_of[0], (LAYER_COUNT, TOKENS, MODEL_WIDTH), 1.0, 6.0, ((0, 4), (1, 2), (2, 4)))
    cotangent = centred(key_of[1], (LAYER_COUNT, TOKENS, MODEL_WIDTH), 1.0, 6.0, ((0, 4), (1, 2), (2, 4)))
    backward_expert_routes_keys = jax.random.split(jax.random.fold_in(key_of[2], 1), LAYER_COUNT * TOKENS // TOK_DEV)
    backward_expert_routes_turns = jax.random.permutation(jax.random.fold_in(key_of[2], 3), LAYER_COUNT * TOKENS // TOK_DEV)
    backward_expert_routes = jax.vmap(lambda own, number: shared_out(jax.random.fold_in(key_of[2], 2), own, number, TOK_DEV, EXPERTS, TOP, CAP, 2))(backward_expert_routes_keys, backward_expert_routes_turns).reshape((LAYER_COUNT, TOKENS, TOP))
    backward_job_lengths = jax.vmap(lambda own: uneven(own, ADAPTER_JOBS, TOKENS, TOKENS // 2, 2))(jax.random.split(key_of[3], LAYER_COUNT)).reshape((LAYER_COUNT, ADAPTER_JOBS)).astype(jnp.int32)
    layer_norm_gains = jnp.clip(1.0 + 0.15 * jax.random.normal(key_of[4], (LAYER_COUNT, MODEL_WIDTH), jnp.float32), 0.25, 1.75)
    router = centred(key_of[5], (LAYER_COUNT, MODEL_WIDTH, EXPERTS), MODEL_WIDTH ** -0.5, 0.125, ((0, 4),))
    expert_gate_weight = centred(key_of[6], (LAYER_COUNT, MODEL_WIDTH, EXPERTS * FF), MODEL_WIDTH ** -0.5, 0.125, ((0, 4), (2, 8)))
    expert_up_weight = centred(key_of[7], (LAYER_COUNT, MODEL_WIDTH, EXPERTS * FF), MODEL_WIDTH ** -0.5, 0.125, ((0, 4), (2, 8)))
    expert_down_weight = centred(key_of[8], (LAYER_COUNT, EXPERTS * FF, MODEL_WIDTH), FF ** -0.5, 0.0625, ((0, 4), (1, 8)))
    adapter_down_maps = centred(key_of[9], (LAYER_COUNT, MODEL_WIDTH, ADAPTER_JOBS * ADAPTER_RANK), MODEL_WIDTH ** -0.5, 0.125, ((0, 4), (1, 4)))
    adapter_up_maps = centred(key_of[10], (LAYER_COUNT, ADAPTER_JOBS * ADAPTER_RANK, MODEL_WIDTH), ADAPTER_RANK ** -0.5, 1.5, ((0, 4), (2, 4)))
    return {"stash": stash, "cotangent": cotangent, "backward_expert_routes": backward_expert_routes, "backward_job_lengths": backward_job_lengths, "layer_norm_gains": layer_norm_gains, "router": router, "expert_gate_weight": expert_gate_weight, "expert_up_weight": expert_up_weight, "expert_down_weight": expert_down_weight, "adapter_down_maps": adapter_down_maps, "adapter_up_maps": adapter_up_maps}


EPS = 1e-05
ADAPTER_SCALE = 0.5
HIGH = lax.Precision.HIGHEST

def job_columns(job_token_lengths, offset, count):
    ends = jnp.cumsum(job_token_lengths, dtype=jnp.int32)
    position = offset + jnp.arange(count, dtype=jnp.int32)
    owner = lax.optimization_barrier(jnp.sum((ends[None, :] <= position[:, None]).astype(jnp.int32), axis=1, dtype=jnp.int32))
    column_owner = jnp.arange(job_token_lengths.shape[0] * ADAPTER_RANK, dtype=jnp.int32) // ADAPTER_RANK
    return (owner[:, None] == column_owner[None, :]).astype(jnp.float32)

def prepare(whole_batch, norm_gain_vector, router, token_routes):
    expert_values = whole_batch.astype(jnp.float32)
    scale = lax.rsqrt(lax.optimization_barrier(jnp.mean(expert_values * expert_values, axis=1, keepdims=True)) + EPS)
    normalized_input = (expert_values * scale * norm_gain_vector[None, :]).astype(jnp.bfloat16)
    logits = jnp.dot(normalized_input, router, preferred_element_type=jnp.float32)
    labels = jnp.arange(router.shape[1], dtype=jnp.int32)
    first = (token_routes[:, 0:1] == labels[None, :]).astype(jnp.float32)
    second = (token_routes[:, 1:2] == labels[None, :]).astype(jnp.float32)
    upper = jax.nn.sigmoid(lax.optimization_barrier(jnp.sum(first * logits, axis=1)) - lax.optimization_barrier(jnp.sum(second * logits, axis=1)))
    table = upper[:, None] * first + (1.0 - upper)[:, None] * second
    return (expert_values, scale, normalized_input, first, second, upper, table)

def router_grad(gate_grad, first, second, upper):
    spread = lax.optimization_barrier(jnp.sum(first * gate_grad, axis=1)) - lax.optimization_barrier(jnp.sum(second * gate_grad, axis=1))
    delta = spread * upper * (1.0 - upper)
    return delta[:, None] * (first - second)

def layer_backward_pass(whole_batch, adapter_gradient_list, norm_gain_vector, router, expert_gate_weight, expert_up_weight, expert_down_weight, adapter_down_maps, adapter_up_maps, token_routes, job_token_lengths):
    expert_values, scale, normalized_input, first, second, upper, table = prepare(whole_batch, norm_gain_vector, router, token_routes)
    grad_values = adapter_gradient_list.astype(jnp.float32)
    job_mask = job_columns(job_token_lengths, 0, expert_values.shape[0])
    low_rank_rows = (jnp.dot(normalized_input, adapter_down_maps, preferred_element_type=jnp.float32) * job_mask).astype(jnp.bfloat16)
    grad_low_rank = (ADAPTER_SCALE * jnp.dot(adapter_gradient_list, adapter_up_maps.T, preferred_element_type=jnp.float32) * job_mask).astype(jnp.bfloat16)
    up_map_gradient = ADAPTER_SCALE * jnp.dot(low_rank_rows.T, adapter_gradient_list, preferred_element_type=jnp.float32)
    down_map_gradient = jnp.dot(normalized_input.T, grad_low_rank, preferred_element_type=jnp.float32)
    grad_normalized = jnp.dot(grad_low_rank, adapter_down_maps.T, preferred_element_type=jnp.float32)
    gate_terms = []
    for expert in range(EXPERTS):
        lower_col = expert * FF
        wg = expert_gate_weight[:, lower_col:lower_col + FF]
        wu = expert_up_weight[:, lower_col:lower_col + FF]
        wd = expert_down_weight[lower_col:lower_col + FF, :]
        gate = jnp.dot(normalized_input, wg, preferred_element_type=jnp.float32)
        up = jnp.dot(normalized_input, wu, preferred_element_type=jnp.float32)
        sig = jax.nn.sigmoid(gate)
        act = gate * sig
        hidden = (act * up).astype(jnp.bfloat16)
        output = jnp.dot(hidden, wd, preferred_element_type=jnp.float32)
        gate_terms.append(lax.optimization_barrier(jnp.sum(grad_values * output, axis=1)))
        back = jnp.dot(adapter_gradient_list, wd.T, preferred_element_type=jnp.float32)
        d_gate = (back * up * sig * (1.0 + gate * (1.0 - sig))).astype(jnp.bfloat16)
        d_up = (back * act).astype(jnp.bfloat16)
        inner = jnp.dot(d_gate, wg.T, preferred_element_type=jnp.float32) + jnp.dot(d_up, wu.T, preferred_element_type=jnp.float32)
        grad_normalized = grad_normalized + table[:, expert:expert + 1] * inner
    gate_grad = jnp.stack(gate_terms, axis=1)
    d_logit = router_grad(gate_grad, first, second, upper)
    grad_normalized = grad_normalized + jnp.dot(d_logit, router.astype(jnp.float32).T, precision=HIGH)
    weighted = grad_normalized * norm_gain_vector[None, :]
    stat = lax.optimization_barrier(jnp.sum(weighted * expert_values, axis=1, keepdims=True))
    layer_result = grad_values + scale * weighted - expert_values * scale * scale * scale * stat / MODEL_WIDTH
    return (layer_result.astype(jnp.bfloat16), down_map_gradient, up_map_gradient)

def reference(stash, cotangent, backward_expert_routes, backward_job_lengths, layer_norm_gains, router, expert_gate_weight, expert_up_weight, expert_down_weight, adapter_down_maps, adapter_up_maps):

    def single_layer_tick(items):
        x_stash, adapter_gradient_list, b_routes, b_lengths, norm_gain_vector, route_w, wg, wu, wd, a_map, b_map = items
        return layer_backward_pass(x_stash, adapter_gradient_list, norm_gain_vector, route_w, wg, wu, wd, a_map, b_map, b_routes, b_lengths)
    backward_outputs, down_map_gradient, up_map_gradient = lax.map(single_layer_tick, (stash, cotangent, backward_expert_routes, backward_job_lengths, layer_norm_gains, router, expert_gate_weight, expert_up_weight, expert_down_weight, adapter_down_maps, adapter_up_maps))
    return (jnp.roll(backward_outputs, -1, axis=0), down_map_gradient, up_map_gradient)
```

```python
import functools

import jax
import jax.numpy as jnp
from jax import lax
from jax.experimental import pallas as pl
from jax.experimental.pallas import tpu as pltpu
from jax.sharding import PartitionSpec as P

ADAPTER_RANK = 16
CAP = 80

EPS = 1e-05
ADAPTER_SCALE = 0.5
MESH = pl.DeviceIdType.MESH
VMEM_LIMIT = 60 * 1024 * 1024
LANES = 128
LAST = (((1,), (1,)), ((), ()))
FIRST = (((0,), (0,)), ((), ()))


def job_columns(job_token_lengths, offset, count):
    ends = jnp.cumsum(job_token_lengths, dtype=jnp.int32)
    position = offset + jnp.arange(count, dtype=jnp.int32)
    owner = jnp.sum((ends[None, :] <= position[:, None]).astype(jnp.int32), axis=1, dtype=jnp.int32)
    column_owner = (
        jnp.arange(job_token_lengths.shape[0] * ADAPTER_RANK, dtype=jnp.int32) // ADAPTER_RANK
    )
    return (owner[:, None] == column_owner[None, :]).astype(jnp.float32)


def greet(targets):
    barrier = pltpu.get_barrier_semaphore()
    for target in targets:
        pl.semaphore_signal(barrier, inc=1, device_id=target, device_id_type=MESH)
    pl.semaphore_wait(barrier, len(targets))


def gather_kernel(
    n, per, rows_ref, stats_ref, lows_ref, rows_out, stats_out, lows_out,
    rs, rr, ss, sr, ls, lr, fs, fr, own,
):
    me = lax.axis_index("expert")
    core = lax.axis_index("dp")
    partner = {"dp": 1 - core}
    peers = [lax.rem(me + k, n) for k in range(1, n)]
    greet([{"expert": peer} for peer in peers] + [partner])

    def send(src, dst, a, b, k, target):
        copy = pltpu.make_async_remote_copy(
            src_ref=src, dst_ref=dst, send_sem=a.at[k], recv_sem=b.at[k],
            device_id=target, device_id_type=MESH,
        )
        copy.start()
        return copy

    rows, small = [], []
    for k, peer in enumerate(peers):
        target = {"expert": peer}
        rows.append(send(rows_ref.at[peer // per], rows_out.at[core, me], rs, rr, k, target))
        small.append(send(stats_ref, stats_out.at[me], ss, sr, k, target))
        small.append(send(lows_ref, lows_out.at[me], ls, lr, k, target))
    mine = rows_ref.at[me // per]
    local = [
        pltpu.make_async_copy(mine, rows_out.at[core, me], own.at[0]),
        pltpu.make_async_copy(stats_ref, stats_out.at[me], own.at[1]),
        pltpu.make_async_copy(lows_ref, lows_out.at[me], own.at[2]),
    ]
    for copy in local:
        copy.start()
    passed = [send(mine, rows_out.at[core, me], fs, fr, n - 1, partner)]
    for k in range(n - 1):
        rows[k].wait_recv()
        origin = lax.rem(me + (n - 1 - k), n)
        landed = rows_out.at[core, origin]
        passed.append(send(landed, landed, fs, fr, k, partner))
    for copy in rows:
        copy.wait_send()
    for copy in small + local + passed:
        copy.wait()


def gather(n, per, shards, rows, stats, lows):
    vmem = pl.BlockSpec(memory_space=pltpu.VMEM)
    dma = pltpu.SemaphoreType.DMA
    return pl.pallas_call(
        functools.partial(gather_kernel, n, per),
        out_shape=(
            jax.ShapeDtypeStruct((shards, n) + rows.shape[1:], rows.dtype),
            jax.ShapeDtypeStruct((n,) + stats.shape, stats.dtype),
            jax.ShapeDtypeStruct((n,) + lows.shape, lows.dtype),
        ),
        in_specs=[vmem] * 3,
        out_specs=(vmem,) * 3,
        scratch_shapes=[dma((n - 1,))] * 6 + [dma((n,))] * 2 + [dma((3,))],
        compiler_params=pltpu.CompilerParams(
            collective_id=0, has_side_effects=True, vmem_limit_bytes=VMEM_LIMIT
        ),
    )(rows, stats, lows)


def expert_kernel(
    n, width, rows_ref, gain_ref, wg_ref, wu_ref, wd_ref, dn_ref, vec_ref, normed, cot, acc, vec
):
    step = pl.program_id(0)
    shards, cap = rows_ref.shape[0], rows_ref.shape[2]

    @pl.when(step == 0)
    def _():
        for s in range(shards):
            r = slice(s * cap, (s + 1) * cap)
            total = jnp.zeros((cap, 1), jnp.float32)
            for j in range(n):
                x = rows_ref[s, j, :, :width].astype(jnp.float32)
                total += jnp.sum(x * x, axis=1, keepdims=True)
            scale = lax.rsqrt(total / (n * width) + EPS)
            for j in range(n):
                c = slice(j * width, (j + 1) * width)
                x = rows_ref[s, j, :, :width].astype(jnp.float32)
                normed[r, c] = (x * scale * gain_ref[:, c]).astype(jnp.bfloat16)
                cot[r, c] = rows_ref[s, j, :, width:]
        acc[...] = jnp.zeros_like(acc)
        vec[...] = jnp.zeros_like(vec)

    x, g = normed[...], cot[...]
    gate = jnp.dot(x, wg_ref[...], preferred_element_type=jnp.float32)
    up = jnp.dot(x, wu_ref[...], preferred_element_type=jnp.float32)
    back = lax.dot_general(g, wd_ref[...], LAST, preferred_element_type=jnp.float32)
    sig = jax.nn.sigmoid(gate)
    act = gate * sig
    d_up = back * act
    d_gate = back * up * sig * (1.0 + gate * (1.0 - sig))
    gate_term = jnp.sum(d_up * up, axis=1, keepdims=True)
    stat_term = jnp.sum(d_gate * gate + d_up * up, axis=1, keepdims=True)
    lane = lax.broadcasted_iota(jnp.int32, vec.shape, 1)
    vec[...] += jnp.where(lane % 2 == 0, gate_term, stat_term)
    acc[...] += lax.dot_general(
        d_gate.astype(jnp.bfloat16), wg_ref[...], LAST, preferred_element_type=jnp.float32
    ) + lax.dot_general(
        d_up.astype(jnp.bfloat16), wu_ref[...], LAST, preferred_element_type=jnp.float32
    )

    @pl.when(step == pl.num_programs(0) - 1)
    def _():
        for s in range(shards):
            r = slice(s * cap, (s + 1) * cap)
            vec_ref[s] = vec[r, :]
            for j in range(n):
                dn_ref[s, j] = acc[r, j * width:(j + 1) * width]


def expert_back(rows, gains, wg, wu, wd):
    shards, n, cap, double = rows.shape
    width = double // 2
    model, hidden = n * width, wg.shape[2]
    tile = next(t for t in (512, 256, 128, hidden) if hidden % t == 0)
    slots = shards * cap
    return pl.pallas_call(
        functools.partial(expert_kernel, n, width),
        grid=(hidden // tile,),
        out_shape=(
            jax.ShapeDtypeStruct((shards, n, cap, width), jnp.float32),
            jax.ShapeDtypeStruct((shards, cap, LANES), jnp.float32),
        ),
        in_specs=[
            pl.BlockSpec(rows.shape, lambda i: (0, 0, 0, 0)),
            pl.BlockSpec((1, model), lambda i: (0, 0)),
            pl.BlockSpec((None, model, tile), lambda i: (0, 0, i)),
            pl.BlockSpec((None, model, tile), lambda i: (0, 0, i)),
            pl.BlockSpec((None, tile, model), lambda i: (0, i, 0)),
        ],
        out_specs=(
            pl.BlockSpec((shards, n, cap, width), lambda i: (0, 0, 0, 0)),
            pl.BlockSpec((shards, cap, LANES), lambda i: (0, 0, 0)),
        ),
        scratch_shapes=[
            pltpu.VMEM((slots, model), jnp.bfloat16),
            pltpu.VMEM((slots, model), jnp.bfloat16),
            pltpu.VMEM((slots, model), jnp.float32),
            pltpu.VMEM((slots, LANES), jnp.float32),
        ],
        compiler_params=pltpu.CompilerParams(
            dimension_semantics=("arbitrary",), vmem_limit_bytes=VMEM_LIMIT
        ),
    )(rows, gains, wg, wu, wd)


def scatter_kernel(
    n, per, experts, sections,
    dn_ref, vec_ref, pd_ref, pu_ref, st_ref, tok_ref, base_ref, x_ref, g_ref, gain_ref, rt_ref,
    back_out, pd_out, pu_out,
    pdn, pvec, ppd, ppu, sendbuf, landing, result, ps, pr, qs, qr, es, er, zs, zr,
):
    me = lax.axis_index("expert")
    core = lax.axis_index("dp")
    sec = lax.axis_index("section")
    other = 1 - core
    partner = {"dp": other}
    width = x_ref.shape[1]
    ahead = {"section": lax.rem(sec + sections - 1, sections)}
    behind = {"section": lax.rem(sec + 1, sections)}
    peers = [lax.rem(me + k, n) for k in range(1, n)]
    greet([{"expert": peer} for peer in peers] + [partner, ahead, behind])

    def send(src, dst, a, b, k, target):
        copy = pltpu.make_async_remote_copy(
            src_ref=src, dst_ref=dst, send_sem=a.at[k], recv_sem=b.at[k],
            device_id=target, device_id_type=MESH,
        )
        copy.start()
        return copy

    shared = [send(vec_ref.at[other], pvec, qs, qr, 0, partner)]
    blocks = [
        send(dn_ref.at[other, peer], pdn.at[k], ps, pr, k, partner)
        for k, peer in enumerate(peers + [me])
    ]
    shared.append(send(pd_ref, ppd, qs, qr, 1, partner))
    shared.append(send(pu_ref, ppu, qs, qr, 2, partner))

    shared[0].wait()
    v = vec_ref[core] + pvec[...]
    high = v.astype(jnp.bfloat16)
    rest = (v - high.astype(jnp.float32)).astype(jnp.bfloat16)
    lane = lax.broadcasted_iota(jnp.int32, v.shape, 1)
    packed = jnp.where(lane < 2, high.astype(jnp.float32), rest.astype(jnp.float32)).astype(
        jnp.bfloat16
    )
    sent = []
    for k, peer in enumerate(peers):
        blocks[k].wait()
        sendbuf[k, :, :width] = (dn_ref[core, peer] + pdn[k]).astype(jnp.bfloat16)
        sendbuf[k, :, width:] = packed
        sent.append(send(sendbuf.at[k], landing.at[k], es, er, k, {"expert": peer}))
    blocks[n - 1].wait()
    own_rows = (dn_ref[core, me] + pdn[n - 1]).astype(jnp.bfloat16)

    token = tok_ref[...]
    column = lambda i: token[:, i:i + 1]
    spread = jnp.zeros_like(column(0))
    stat = jnp.zeros_like(spread)
    total = base_ref[...]

    def pick(ref_index, values):
        return jnp.dot(st_ref[ref_index], values, preferred_element_type=jnp.float32)

    def weights_of(expert):
        gate, sign = jnp.zeros_like(spread), jnp.zeros_like(spread)
        for e in range(experts):
            mark = (expert == e).astype(jnp.float32)
            gate += mark * column(e)
            sign += mark * column(experts + e)
        return gate, sign

    def add(expert, row_part, vec_part, total, spread, stat):
        gate, sign = weights_of(expert)
        picked = pick(expert, vec_part)
        spread = spread + sign * (picked[:, 0:1] + picked[:, 2:3])
        stat = stat + gate * (picked[:, 1:2] + picked[:, 3:4])
        return total + gate * pick(expert, row_part), spread, stat

    total, spread, stat = add(me // per, own_rows, packed, total, spread, stat)
    for k in range(n - 1):
        sent[k].wait()
        expert = lax.rem(me + (n - 1 - k), n) // per
        total, spread, stat = add(
            expert, landing[k, :, :width], landing[k, :, width:], total, spread, stat
        )
    scale = column(2 * experts + 1)
    delta = spread * column(2 * experts)
    for e in range(experts):
        total = total + (delta * column(experts + e)) * rt_ref[e:e + 1, :]
    stat = stat / scale + column(2 * experts + 2) + delta * column(2 * experts + 3)
    x = x_ref[...].astype(jnp.float32)
    g = g_ref[...].astype(jnp.float32)
    weighted = total * gain_ref[...]
    out = g + scale * weighted - x * (scale * scale * scale * stat / (n * width))
    result[...] = out.astype(jnp.bfloat16)
    handed = send(result, back_out, zs, zr, 0, ahead)
    shared[1].wait()
    pd_out[...] = pd_ref[...] + ppd[...]
    shared[2].wait()
    pu_out[...] = pu_ref[...] + ppu[...]
    handed.wait()


def scatter(n, per, experts, sections, dn, vec, pd, pu, *rest):
    cap, width = dn.shape[2:]
    x = rest[3]
    vmem = pl.BlockSpec(memory_space=pltpu.VMEM)
    dma = pltpu.SemaphoreType.DMA
    return pl.pallas_call(
        functools.partial(scatter_kernel, n, per, experts, sections),
        out_shape=(
            jax.ShapeDtypeStruct(x.shape, jnp.bfloat16),
            jax.ShapeDtypeStruct(pd.shape, jnp.float32),
            jax.ShapeDtypeStruct(pu.shape, jnp.float32),
        ),
        in_specs=[vmem] * (4 + len(rest)),
        out_specs=(vmem,) * 3,
        scratch_shapes=[
            pltpu.VMEM((n, cap, width), jnp.float32),
            pltpu.VMEM(vec.shape[1:], jnp.float32),
            pltpu.VMEM(pd.shape, jnp.float32),
            pltpu.VMEM(pu.shape, jnp.float32),
            pltpu.VMEM((n - 1, cap, width + LANES), jnp.bfloat16),
            pltpu.VMEM((n - 1, cap, width + LANES), jnp.bfloat16),
            pltpu.VMEM(x.shape, jnp.bfloat16),
            dma((n,)), dma((n,)), dma((3,)), dma((3,)),
            dma((n - 1,)), dma((n - 1,)), dma((1,)), dma((1,)),
        ],
        compiler_params=pltpu.CompilerParams(
            collective_id=1, has_side_effects=True, vmem_limit_bytes=VMEM_LIMIT
        ),
    )(dn, vec, pd, pu, *rest)


def body(
    stash,
    cotangent,
    backward_expert_routes,
    backward_job_lengths,
    layer_norm_gains,
    router,
    expert_gate_weight,
    expert_up_weight,
    expert_down_weight,
    adapter_down_maps,
    adapter_up_maps,
):
    n = lax.axis_size("expert")
    shards = lax.axis_size("dp")
    sections = lax.axis_size("section")
    experts = router.shape[2]
    per = n // experts
    me = lax.axis_index("expert")
    x, g = stash[0], cotangent[0]
    count, width = x.shape
    routes = backward_expert_routes[0]
    gain = lax.dynamic_slice_in_dim(layer_norm_gains, me * width, width, 1)
    route_cols = lax.dynamic_slice_in_dim(router[0], me * width, width, 0)
    down, up_map = adapter_down_maps[0], adapter_up_maps[0]
    ranks = down.shape[1]

    labels = jnp.arange(experts, dtype=jnp.int32)
    first = (routes[:, 0:1] == labels[None, :]).astype(jnp.float32)
    second = (routes[:, 1:2] == labels[None, :]).astype(jnp.float32)
    member = first + second
    order = jnp.arange(count, dtype=jnp.int32)
    before = (order[None, :] < order[:, None]).astype(jnp.bfloat16)
    rank = jnp.dot(before, member.astype(jnp.bfloat16), preferred_element_type=jnp.float32)
    place = jnp.where(member > 0, rank, -1.0)
    slots = jnp.arange(CAP, dtype=jnp.float32)
    spread_to = (place.T[:, :, None] == slots[None, None, :]).astype(jnp.bfloat16)
    select = (place.T[:, None, :] == slots[None, :, None]).astype(jnp.bfloat16)

    both = jnp.concatenate([x, g], axis=1)
    rows = jnp.dot(
        select.reshape(experts * CAP, count), both, preferred_element_type=jnp.float32
    ).astype(jnp.bfloat16).reshape(experts, CAP, 2 * width)
    xf = x.astype(jnp.float32)
    gained = (xf * gain).astype(jnp.bfloat16)
    square = jnp.sum(xf * xf, axis=1)[None, :]
    raw = lax.dot_general(
        route_cols, gained, (((0,), (1,)), ((), ())), preferred_element_type=jnp.float32
    )
    fill = -(1 + experts) % 8
    stats = jnp.concatenate([square, raw, jnp.zeros((fill, count), jnp.float32)], axis=0)
    lows = jnp.concatenate(
        [
            jnp.dot(gained, down, preferred_element_type=jnp.float32),
            lax.dot_general(g, up_map, LAST, preferred_element_type=jnp.float32),
        ],
        axis=1,
    ).astype(jnp.bfloat16)

    all_rows, all_stats, all_lows = gather(n, per, shards, rows, stats, lows)

    dn, vec = expert_back(
        all_rows, layer_norm_gains, expert_gate_weight, expert_up_weight, expert_down_weight
    )

    stat = jnp.sum(all_stats, axis=0).T
    scale = lax.rsqrt(stat[:, 0:1] / (n * width) + EPS)
    raw_logits = stat[:, 1:1 + experts]
    sign = first - second
    raw_spread = jnp.sum(sign * raw_logits, axis=1, keepdims=True)
    upper = jax.nn.sigmoid(raw_spread * scale)
    table = upper * first + (1.0 - upper) * second
    low_all = jnp.sum(all_lows.astype(jnp.float32), axis=0)
    raw_low, g_low = low_all[:, :ranks], low_all[:, ranks:]
    mask = job_columns(backward_job_lengths[0], lax.axis_index("dp") * count, count)
    low = (raw_low * scale * mask).astype(jnp.bfloat16)
    d_low = (ADAPTER_SCALE * g_low * mask).astype(jnp.bfloat16)
    normed_cols = (xf * scale * gain).astype(jnp.bfloat16)
    pu = ADAPTER_SCALE * lax.dot_general(low, g, FIRST, preferred_element_type=jnp.float32)
    pd = lax.dot_general(normed_cols, d_low, FIRST, preferred_element_type=jnp.float32)
    base = lax.dot_general(d_low, down, LAST, preferred_element_type=jnp.float32)
    low_stat = jnp.sum(d_low.astype(jnp.float32) * raw_low, axis=1, keepdims=True)
    columns = [table, sign, upper * (1.0 - upper), scale, low_stat, raw_spread]
    used = sum(c.shape[1] for c in columns)
    token = jnp.concatenate(columns + [jnp.zeros((count, -used % LANES), jnp.float32)], axis=1)

    handed_back, down_grad, up_grad = scatter(
        n, per, experts, sections, dn, vec, pd, pu,
        spread_to, token, base, x, g, gain, route_cols.astype(jnp.float32).T,
    )
    return (handed_back[None], down_grad[None], up_grad[None])


def solution(mesh):
    return jax.shard_map(
        body,
        mesh=mesh,
        in_specs=(
            P("section", "dp", "expert"),
            P("section", "dp", "expert"),
            P("section", "dp", None),
            P("section", None),
            P("section", None),
            P("section", None, None),
            P("section", None, ("expert", "dp")),
            P("section", None, ("expert", "dp")),
            P("section", ("expert", "dp"), None),
            P("section", "expert", None),
            P("section", None, "expert"),
        ),
        out_specs=(
            P("section", "dp", "expert"),
            P("section", "expert", None),
            P("section", None, "expert"),
        ),
        check_vma=False,
    )
```

```python
import functools

import jax
import jax.numpy as jnp
from jax import lax
from jax.experimental import pallas as pl
from jax.experimental.pallas import tpu as pltpu
from jax.sharding import PartitionSpec as P

ADAPTER_RANK = 16
CAP = 80

EPS = 1e-05
ADAPTER_SCALE = 0.5
MESH = pl.DeviceIdType.MESH
VMEM_LIMIT = 60 * 1024 * 1024
LANES = 128
LAST = (((1,), (1,)), ((), ()))
FIRST = (((0,), (0,)), ((), ()))


def job_columns(job_token_lengths, offset, count):
    ends = jnp.cumsum(job_token_lengths, dtype=jnp.int32)
    position = offset + jnp.arange(count, dtype=jnp.int32)
    owner = jnp.sum((ends[None, :] <= position[:, None]).astype(jnp.int32), axis=1, dtype=jnp.int32)
    column_owner = (
        jnp.arange(job_token_lengths.shape[0] * ADAPTER_RANK, dtype=jnp.int32) // ADAPTER_RANK
    )
    return (owner[:, None] == column_owner[None, :]).astype(jnp.float32)


def greet(targets):
    barrier = pltpu.get_barrier_semaphore()
    for target in targets:
        pl.semaphore_signal(barrier, inc=1, device_id=target, device_id_type=MESH)
    pl.semaphore_wait(barrier, len(targets))


def gather_kernel(
    n, per, select_ref, x_ref, g_ref, gain_ref, route_ref, down_ref, up_ref,
    rows_out, stats_out, lows_out, rows_ref, stats_ref, lows_ref, rs, rr, ss, sr, ls, lr, fs, fr, own,
):
    me = lax.axis_index("expert")
    core = lax.axis_index("dp")
    partner = {"dp": 1 - core}
    peers = [lax.rem(me + k, n) for k in range(1, n)]
    greet([{"expert": peer} for peer in peers] + [partner])

    def send(src, dst, a, b, k, target):
        copy = pltpu.make_async_remote_copy(
            src_ref=src, dst_ref=dst, send_sem=a.at[k], recv_sem=b.at[k],
            device_id=target, device_id_type=MESH,
        )
        copy.start()
        return copy

    width = x_ref.shape[1]
    x, g = x_ref[...], g_ref[...]
    for e in range(select_ref.shape[0]):
        chosen = select_ref[e]
        rows_ref[e, :, :width] = jnp.dot(chosen, x, preferred_element_type=jnp.float32).astype(
            jnp.bfloat16
        )
        rows_ref[e, :, width:] = jnp.dot(chosen, g, preferred_element_type=jnp.float32).astype(
            jnp.bfloat16
        )
    rows, small = [], []
    for k, peer in enumerate(peers):
        target = {"expert": peer}
        rows.append(send(rows_ref.at[peer // per], rows_out.at[core, me], rs, rr, k, target))
    xf = x.astype(jnp.float32)
    gained = (xf * gain_ref[...]).astype(jnp.bfloat16)
    raw = lax.dot_general(route_ref[...], gained, LAST, preferred_element_type=jnp.float32)
    square = lax.dot_general(
        jnp.ones(route_ref.shape, jnp.float32), xf * xf, LAST,
        precision=lax.Precision.HIGHEST, preferred_element_type=jnp.float32,
    )
    line = lax.broadcasted_iota(jnp.int32, raw.shape, 0)
    stats_ref[...] = jnp.where(line == 0, square, raw)
    lows_ref[...] = jnp.concatenate(
        [
            jnp.dot(gained, down_ref[...], preferred_element_type=jnp.float32),
            lax.dot_general(g, up_ref[...], LAST, preferred_element_type=jnp.float32),
        ],
        axis=1,
    ).astype(jnp.bfloat16)
    for k, peer in enumerate(peers):
        target = {"expert": peer}
        small.append(send(stats_ref, stats_out.at[me], ss, sr, k, target))
        small.append(send(lows_ref, lows_out.at[me], ls, lr, k, target))
    mine = rows_ref.at[me // per]
    local = [
        pltpu.make_async_copy(mine, rows_out.at[core, me], own.at[0]),
        pltpu.make_async_copy(stats_ref, stats_out.at[me], own.at[1]),
        pltpu.make_async_copy(lows_ref, lows_out.at[me], own.at[2]),
    ]
    for copy in local:
        copy.start()
    passed = [send(mine, rows_out.at[core, me], fs, fr, n - 1, partner)]
    for k in range(n - 1):
        rows[k].wait_recv()
        origin = lax.rem(me + (n - 1 - k), n)
        landed = rows_out.at[core, origin]
        passed.append(send(landed, landed, fs, fr, k, partner))
    for copy in rows:
        copy.wait_send()
    for copy in small + local + passed:
        copy.wait()


def gather(n, per, shards, select, x, g, gain, route, down, up):
    count, width = x.shape
    rows = jax.ShapeDtypeStruct(select.shape[:2] + (2 * width,), x.dtype)
    stats = jax.ShapeDtypeStruct((route.shape[0], count), jnp.float32)
    lows = jax.ShapeDtypeStruct((count, 2 * down.shape[1]), x.dtype)
    vmem = pl.BlockSpec(memory_space=pltpu.VMEM)
    dma = pltpu.SemaphoreType.DMA
    return pl.pallas_call(
        functools.partial(gather_kernel, n, per),
        out_shape=(
            jax.ShapeDtypeStruct((shards, n) + rows.shape[1:], rows.dtype),
            jax.ShapeDtypeStruct((n,) + stats.shape, stats.dtype),
            jax.ShapeDtypeStruct((n,) + lows.shape, lows.dtype),
        ),
        in_specs=[vmem] * 7,
        out_specs=(vmem,) * 3,
        scratch_shapes=[pltpu.VMEM(a.shape, a.dtype) for a in (rows, stats, lows)] + [dma((n - 1,))] * 6 + [dma((n,))] * 2 + [dma((3,))],
        compiler_params=pltpu.CompilerParams(
            collective_id=0, has_side_effects=True, vmem_limit_bytes=VMEM_LIMIT
        ),
    )(select, x, g, gain, route, down, up)


def expert_kernel(
    n, width, rows_ref, gain_ref, wg_ref, wu_ref, wd_ref, dn_ref, vec_ref, normed, cot, acc, vec
):
    step = pl.program_id(0)
    shards, cap = rows_ref.shape[0], rows_ref.shape[2]

    @pl.when(step == 0)
    def _():
        for s in range(shards):
            r = slice(s * cap, (s + 1) * cap)
            total = jnp.zeros((cap, 1), jnp.float32)
            for j in range(n):
                x = rows_ref[s, j, :, :width].astype(jnp.float32)
                total += jnp.sum(x * x, axis=1, keepdims=True)
            scale = lax.rsqrt(total / (n * width) + EPS)
            for j in range(n):
                c = slice(j * width, (j + 1) * width)
                x = rows_ref[s, j, :, :width].astype(jnp.float32)
                normed[r, c] = (x * scale * gain_ref[:, c]).astype(jnp.bfloat16)
                cot[r, c] = rows_ref[s, j, :, width:]
        acc[...] = jnp.zeros_like(acc)
        vec[...] = jnp.zeros_like(vec)

    x, g = normed[...], cot[...]
    gate = jnp.dot(x, wg_ref[...], preferred_element_type=jnp.float32)
    up = jnp.dot(x, wu_ref[...], preferred_element_type=jnp.float32)
    back = lax.dot_general(g, wd_ref[...], LAST, preferred_element_type=jnp.float32)
    sig = jax.nn.sigmoid(gate)
    act = gate * sig
    d_up = back * act
    d_gate = back * up * sig * (1.0 + gate * (1.0 - sig))
    gate_term = jnp.sum(d_up * up, axis=1, keepdims=True)
    stat_term = jnp.sum(d_gate * gate + d_up * up, axis=1, keepdims=True)
    lane = lax.broadcasted_iota(jnp.int32, vec.shape, 1)
    vec[...] += jnp.where(lane % 2 == 0, gate_term, stat_term)
    acc[...] += lax.dot_general(
        d_gate.astype(jnp.bfloat16), wg_ref[...], LAST, preferred_element_type=jnp.float32
    ) + lax.dot_general(
        d_up.astype(jnp.bfloat16), wu_ref[...], LAST, preferred_element_type=jnp.float32
    )

    @pl.when(step == pl.num_programs(0) - 1)
    def _():
        for s in range(shards):
            r = slice(s * cap, (s + 1) * cap)
            vec_ref[s] = vec[r, :]
            for j in range(n):
                dn_ref[s, j] = acc[r, j * width:(j + 1) * width]


def expert_back(rows, gains, wg, wu, wd):
    shards, n, cap, double = rows.shape
    width = double // 2
    model, hidden = n * width, wg.shape[2]
    tile = next(t for t in (512, 256, 128, hidden) if hidden % t == 0)
    slots = shards * cap
    return pl.pallas_call(
        functools.partial(expert_kernel, n, width),
        grid=(hidden // tile,),
        out_shape=(
            jax.ShapeDtypeStruct((shards, n, cap, width), jnp.float32),
            jax.ShapeDtypeStruct((shards, cap, LANES), jnp.float32),
        ),
        in_specs=[
            pl.BlockSpec(rows.shape, lambda i: (0, 0, 0, 0)),
            pl.BlockSpec((1, model), lambda i: (0, 0)),
            pl.BlockSpec((None, model, tile), lambda i: (0, 0, i)),
            pl.BlockSpec((None, model, tile), lambda i: (0, 0, i)),
            pl.BlockSpec((None, tile, model), lambda i: (0, i, 0)),
        ],
        out_specs=(
            pl.BlockSpec((shards, n, cap, width), lambda i: (0, 0, 0, 0)),
            pl.BlockSpec((shards, cap, LANES), lambda i: (0, 0, 0)),
        ),
        scratch_shapes=[
            pltpu.VMEM((slots, model), jnp.bfloat16),
            pltpu.VMEM((slots, model), jnp.bfloat16),
            pltpu.VMEM((slots, model), jnp.float32),
            pltpu.VMEM((slots, LANES), jnp.float32),
        ],
        compiler_params=pltpu.CompilerParams(
            dimension_semantics=("arbitrary",), vmem_limit_bytes=VMEM_LIMIT
        ),
    )(rows, gains, wg, wu, wd)


def scatter_kernel(
    n, per, experts, sections,
    dn_ref, vec_ref, select_ref, tok_ref, lows_ref, mask_ref, x_ref, g_ref, gain_ref, rt_ref,
    down_ref,
    back_out, pd_out, pu_out,
    pd_ref, pu_ref, pdn, pvec, ppd, ppu, sendbuf, landing, result, ps, pr, qs, qr, es, er, zs, zr,
):
    me = lax.axis_index("expert")
    core = lax.axis_index("dp")
    sec = lax.axis_index("section")
    other = 1 - core
    partner = {"dp": other}
    width = x_ref.shape[1]
    ahead = {"section": lax.rem(sec + sections - 1, sections)}
    behind = {"section": lax.rem(sec + 1, sections)}
    peers = [lax.rem(me + k, n) for k in range(1, n)]
    greet([{"expert": peer} for peer in peers] + [partner, ahead, behind])

    def send(src, dst, a, b, k, target):
        copy = pltpu.make_async_remote_copy(
            src_ref=src, dst_ref=dst, send_sem=a.at[k], recv_sem=b.at[k],
            device_id=target, device_id_type=MESH,
        )
        copy.start()
        return copy

    shared = [send(vec_ref.at[other], pvec, qs, qr, 0, partner)]
    blocks = [
        send(dn_ref.at[other, peer], pdn.at[k], ps, pr, k, partner)
        for k, peer in enumerate(peers + [me])
    ]
    shared[0].wait()
    v = vec_ref[core] + pvec[...]
    high = v.astype(jnp.bfloat16)
    rest = (v - high.astype(jnp.float32)).astype(jnp.bfloat16)
    lane = lax.broadcasted_iota(jnp.int32, v.shape, 1)
    packed = jnp.where(lane < 2, high.astype(jnp.float32), rest.astype(jnp.float32)).astype(
        jnp.bfloat16
    )
    sent = []
    for k, peer in enumerate(peers):
        blocks[k].wait()
        sendbuf[k, :, :width] = (dn_ref[core, peer] + pdn[k]).astype(jnp.bfloat16)
        sendbuf[k, :, width:] = packed
        sent.append(send(sendbuf.at[k], landing.at[k], es, er, k, {"expert": peer}))
    blocks[n - 1].wait()
    own_rows = (dn_ref[core, me] + pdn[n - 1]).astype(jnp.bfloat16)

    token = tok_ref[...]
    column = lambda i: token[:, i:i + 1]
    scale = column(2 * experts + 1)
    x = x_ref[...].astype(jnp.float32)
    ranks = down_ref.shape[1]
    low_all = lows_ref[0].astype(jnp.float32)
    for j in range(1, n):
        low_all = low_all + lows_ref[j].astype(jnp.float32)
    raw_low, g_low = low_all[:, :ranks], low_all[:, ranks:]
    mask = mask_ref[...]
    low = (raw_low * scale * mask).astype(jnp.bfloat16)
    d_low = (ADAPTER_SCALE * g_low * mask).astype(jnp.bfloat16)
    normed = (x * scale * gain_ref[...]).astype(jnp.bfloat16)
    pd_ref[...] = lax.dot_general(normed, d_low, FIRST, preferred_element_type=jnp.float32)
    pu_ref[...] = ADAPTER_SCALE * lax.dot_general(
        low, g_ref[...], FIRST, preferred_element_type=jnp.float32
    )
    shared.append(send(pd_ref, ppd, qs, qr, 1, partner))
    shared.append(send(pu_ref, ppu, qs, qr, 2, partner))
    low_stat = jnp.sum(d_low.astype(jnp.float32) * raw_low, axis=1, keepdims=True)
    spread = jnp.zeros_like(column(0))
    stat = jnp.zeros_like(spread)
    total = lax.dot_general(d_low, down_ref[...], LAST, preferred_element_type=jnp.float32)

    def pick(ref_index, values):
        return lax.dot_general(
            select_ref[ref_index], values, FIRST, preferred_element_type=jnp.float32
        )

    def weights_of(expert):
        gate, sign = jnp.zeros_like(spread), jnp.zeros_like(spread)
        for e in range(experts):
            mark = (expert == e).astype(jnp.float32)
            gate += mark * column(e)
            sign += mark * column(experts + e)
        return gate, sign

    def add(expert, row_part, vec_part, total, spread, stat):
        gate, sign = weights_of(expert)
        picked = pick(expert, vec_part)
        spread = spread + sign * (picked[:, 0:1] + picked[:, 2:3])
        stat = stat + gate * (picked[:, 1:2] + picked[:, 3:4])
        return total + gate * pick(expert, row_part), spread, stat

    total, spread, stat = add(me // per, own_rows, packed, total, spread, stat)
    for k in range(n - 1):
        sent[k].wait()
        expert = lax.rem(me + (n - 1 - k), n) // per
        total, spread, stat = add(
            expert, landing[k, :, :width], landing[k, :, width:], total, spread, stat
        )
    delta = spread * column(2 * experts)
    for e in range(experts):
        total = total + (delta * column(experts + e)) * rt_ref[e + 1:e + 2, :].astype(
            jnp.float32
        )
    stat = stat / scale + low_stat + delta * column(2 * experts + 2)
    g = g_ref[...].astype(jnp.float32)
    weighted = total * gain_ref[...]
    out = g + scale * weighted - x * (scale * scale * scale * stat / (n * width))
    result[...] = out.astype(jnp.bfloat16)
    handed = send(result, back_out, zs, zr, 0, ahead)
    shared[1].wait()
    pd_out[...] = pd_ref[...] + ppd[...]
    shared[2].wait()
    pu_out[...] = pu_ref[...] + ppu[...]
    handed.wait()


def scatter(n, per, experts, sections, dn, vec, *rest):
    cap, width = dn.shape[2:]
    x, down = rest[4], rest[8]
    pd = jax.ShapeDtypeStruct(down.shape, jnp.float32)
    pu = jax.ShapeDtypeStruct(down.shape[::-1], jnp.float32)
    vmem = pl.BlockSpec(memory_space=pltpu.VMEM)
    dma = pltpu.SemaphoreType.DMA
    return pl.pallas_call(
        functools.partial(scatter_kernel, n, per, experts, sections),
        out_shape=(
            jax.ShapeDtypeStruct(x.shape, jnp.bfloat16),
            jax.ShapeDtypeStruct(pd.shape, jnp.float32),
            jax.ShapeDtypeStruct(pu.shape, jnp.float32),
        ),
        in_specs=[vmem] * (2 + len(rest)),
        out_specs=(vmem,) * 3,
        scratch_shapes=[
            pltpu.VMEM(pd.shape, jnp.float32),
            pltpu.VMEM(pu.shape, jnp.float32),
            pltpu.VMEM((n, cap, width), jnp.float32),
            pltpu.VMEM(vec.shape[1:], jnp.float32),
            pltpu.VMEM(pd.shape, jnp.float32),
            pltpu.VMEM(pu.shape, jnp.float32),
            pltpu.VMEM((n - 1, cap, width + LANES), jnp.bfloat16),
            pltpu.VMEM((n - 1, cap, width + LANES), jnp.bfloat16),
            pltpu.VMEM(x.shape, jnp.bfloat16),
            dma((n,)), dma((n,)), dma((3,)), dma((3,)),
            dma((n - 1,)), dma((n - 1,)), dma((1,)), dma((1,)),
        ],
        compiler_params=pltpu.CompilerParams(
            collective_id=1, has_side_effects=True, vmem_limit_bytes=VMEM_LIMIT
        ),
    )(dn, vec, *rest)


def body(
    stash,
    cotangent,
    backward_expert_routes,
    backward_job_lengths,
    layer_norm_gains,
    router,
    expert_gate_weight,
    expert_up_weight,
    expert_down_weight,
    adapter_down_maps,
    adapter_up_maps,
):
    n = lax.axis_size("expert")
    shards = lax.axis_size("dp")
    sections = lax.axis_size("section")
    experts = router.shape[2]
    per = n // experts
    me = lax.axis_index("expert")
    x, g = stash[0], cotangent[0]
    count, width = x.shape
    routes = backward_expert_routes[0]
    gain = lax.dynamic_slice_in_dim(layer_norm_gains, me * width, width, 1)
    route_cols = lax.dynamic_slice_in_dim(router[0], me * width, width, 0)
    down, up_map = adapter_down_maps[0], adapter_up_maps[0]
    ranks = down.shape[1]

    labels = jnp.arange(experts, dtype=jnp.int32)
    first = (routes[:, 0:1] == labels[None, :]).astype(jnp.float32)
    second = (routes[:, 1:2] == labels[None, :]).astype(jnp.float32)
    member = first + second
    order = jnp.arange(count, dtype=jnp.int32)
    before = (order[None, :] < order[:, None]).astype(jnp.bfloat16)
    rank = jnp.dot(before, member.astype(jnp.bfloat16), preferred_element_type=jnp.float32)
    place = jnp.where(member > 0, rank, -1.0)
    slots = jnp.arange(CAP, dtype=jnp.float32)
    select = (place.T[:, None, :] == slots[None, :, None]).astype(jnp.bfloat16)

    route_t = jnp.pad(route_cols.T, ((1, -(1 + experts) % 8), (0, 0)))

    all_rows, all_stats, all_lows = gather(
        n, per, shards, select, x, g, gain, route_t, down, up_map
    )

    dn, vec = expert_back(
        all_rows, layer_norm_gains, expert_gate_weight, expert_up_weight, expert_down_weight
    )

    stat = jnp.sum(all_stats, axis=0).T
    scale = lax.rsqrt(stat[:, 0:1] / (n * width) + EPS)
    raw_logits = stat[:, 1:1 + experts]
    sign = first - second
    raw_spread = jnp.sum(sign * raw_logits, axis=1, keepdims=True)
    upper = jax.nn.sigmoid(raw_spread * scale)
    table = upper * first + (1.0 - upper) * second
    mask = job_columns(backward_job_lengths[0], lax.axis_index("dp") * count, count)
    columns = [table, sign, upper * (1.0 - upper), scale, raw_spread]
    used = sum(c.shape[1] for c in columns)
    token = jnp.concatenate(columns + [jnp.zeros((count, -used % LANES), jnp.float32)], axis=1)

    handed_back, down_grad, up_grad = scatter(
        n, per, experts, sections, dn, vec, select, token, all_lows, mask, x, g, gain, route_t,
        down,
    )
    return (handed_back[None], down_grad[None], up_grad[None])


def solution(mesh):
    return jax.shard_map(
        body,
        mesh=mesh,
        in_specs=(
            P("section", "dp", "expert"),
            P("section", "dp", "expert"),
            P("section", "dp", None),
            P("section", None),
            P("section", None),
            P("section", None, None),
            P("section", None, ("expert", "dp")),
            P("section", None, ("expert", "dp")),
            P("section", ("expert", "dp"), None),
            P("section", "expert", None),
            P("section", None, "expert"),
        ),
        out_specs=(
            P("section", "dp", "expert"),
            P("section", "expert", None),
            P("section", None, "expert"),
        ),
        check_vma=False,
    )
```
